32 devices in a mesh: wide: 8 (over z, core), narrow: 4 (over y, x).
Axes of the slice: x: 2, y: 2, z: 4, core: 2. Of those that a mesh axis runs over, the one named last changes fastest.
Arguments:
- points: float32 [8192, 128], P(('wide', 'narrow')), may hold values from -6 to 6
- targets: float32 [16, 8192], P(None, ('wide', 'narrow')), may hold values from -6 to 6
- start: float32 [16, 8192], P(None, ('wide', 'narrow')), may hold values from -6 to 6
- interp: float32 [8192, 128], P(('wide', 'narrow')), may hold values from -0.375 to 0.375
- skel_points: float32 [1024, 128], P('wide'), may hold values from -6 to 6
- near_leaves: int32 [64, 8], P(('wide', 'narrow')), may hold values from 0 to 7, as said below
- near_count: int32 [64], P(('wide', 'narrow')), may hold values from 1 to 8
Outputs:
- weights: float32 [16, 8192], P(None, ('wide', 'narrow'))
- residual: float32 [16, 8192], P(None, ('wide', 'narrow'))
The draws below stay inside these ranges and needn't reach their ends.
Inputs may be any that keep to these rules, and one draw needn't show every extreme that they name: `near_leaves`: each row names 8 different leaves of the row's own subtree.
All inputs are finite; a program needn't handle non-finite values.
Results may differ from the reference program's by a relative error of at most 0.0003.
Values sent between devices are 32-bit elements; how exact they have to be, the bound alone decides.
No kernel may reach another device: no remote copies, remote signals or barrier semaphores. Data moves between devices by JAX's collectives and lax.ppermute only.
A program may use at most 64 MiB of HBM per device.

```python
import jax
import jax.numpy as jnp
from jax import lax

DIM = 128
RHS = 16
LEAF = 128
RANK = 128
NEAR = 8
ITERS = 2
LEAF_DEV = 2
LEAVES = 64
POINTS = 8192
NODE_PTS = 1024
SKELETONS = 1024
N_WIDE = 8
N_NARROW = 4


def draw_near_leaves(key, part):
    subtree_size = LEAF_DEV * N_NARROW
    scores = jax.random.randint(key, (LEAVES, subtree_size), 0, 1 << 20, dtype=jnp.int32)
    scores = scores * subtree_size + jnp.arange(subtree_size, dtype=jnp.int32)[None, :]
    ranked = jnp.argsort(scores, axis=1, stable=True)
    return ranked[:, :NEAR].astype(jnp.int32)


def with_ends(drawn, key, least, high):
    place = [jax.random.randint(jax.random.fold_in(key, axis), (), 0, length) for axis, length in enumerate(drawn.shape)]
    main_axis = drawn.shape.index(max(drawn.shape))
    neighbour = place[:main_axis] + [(place[main_axis] + 1) % drawn.shape[main_axis]] + place[main_axis + 1:]
    return drawn.at[tuple(place)].set(least).at[tuple(neighbour)].set(high)


def raised(entries, own_key, source, target, parts, factor):
    def block_of(axis_at):
        return (jnp.arange(entries.shape[axis_at]) // (entries.shape[axis_at] // parts)).reshape((-1,) + (1,) * (entries.ndim - 1 - axis_at))

    near = jax.random.permutation(own_key, parts)[block_of(target)]
    other_side = (block_of(target) + parts // 2) % parts
    return jnp.where((block_of(source) == near) | (block_of(source) == other_side), factor * entries, entries)


def shard_levels(key, dims, pieces, smallest, top_value):
    def one(position, blocks):
        steps = jax.random.uniform(jax.random.fold_in(jax.random.fold_in(key, 6), position), (blocks,), jnp.float32, smallest / len(pieces), top_value / len(pieces))
        return jnp.repeat(jnp.exp(steps), dims[position] // blocks).reshape((-1,) + (1,) * (len(dims) - position - 1))

    loudness = one(*pieces[0])
    for cut in pieces[1:]:
        loudness = loudness * one(*cut)
    return loudness


def bell_draw(rng, extent, spread, limit, shards=(), kind=jnp.bfloat16):
    gain = shard_levels(rng, extent, shards, -0.22, 0.18) if shards else 1.0
    entries = jax.random.normal(rng, extent, jnp.float32) * spread * gain
    return jnp.minimum(jnp.maximum(entries, -limit), limit).astype(kind)


def bell_draw_with(rng, shape, deviation, limit, split, heavy, held_as=jnp.bfloat16):
    drawn = deviation * jax.random.normal(rng, shape, jnp.float32)
    if split:
        drawn = drawn * shard_levels(rng, shape, split, -0.22, 0.18)
    return jnp.clip(raised(drawn, jax.random.fold_in(rng, 3), *heavy), -limit, limit).astype(held_as)


def setup_inputs(seed: int = 0) -> dict:
    arg_keys = jax.random.split(jax.random.key(seed), 8)
    points = bell_draw(arg_keys[0], (POINTS, DIM), 1.0, 6.0, ((0, 32),), jnp.float32)
    targets = bell_draw(arg_keys[1], (RHS, POINTS), 1.0, 6.0, ((1, 32),), jnp.float32)
    start = bell_draw(arg_keys[2], (RHS, POINTS), 1.0, 6.0, ((1, 32),), jnp.float32)
    interp = bell_draw_with(arg_keys[3], (POINTS, RANK), NODE_PTS ** -0.5, 0.375, ((0, 32),), (0, 1, 32, 2.75), jnp.float32)
    skel_points = bell_draw(arg_keys[4], (SKELETONS, DIM), 1.0, 6.0, ((0, 8),), jnp.float32)
    near_leaves = draw_near_leaves(jax.random.fold_in(arg_keys[7], 71), 0)
    near_count = with_ends(jax.random.randint(arg_keys[6], (LEAVES,), 1, NEAR + 1), jax.random.fold_in(arg_keys[6], 1), 1, NEAR).astype(jnp.int32)
    return {"points": points, "targets": targets, "start": start, "interp": interp, "skel_points": skel_points, "near_leaves": near_leaves, "near_count": near_count}


ridge_shift = 1.0
step_size = 0.05
kernel_rate = 2.0
highest = lax.Precision.HIGHEST


def kernel(left_points, right_points):
    cross_prod = jnp.dot(left_points, right_points.T, precision=highest, preferred_element_type=jnp.float32)
    left_sq = jnp.sum(left_points * left_points, axis=1)
    right_sq = jnp.sum(right_points * right_points, axis=1)
    return jnp.exp(-(kernel_rate / DIM) * (left_sq[:, None] + right_sq[None, :] - 2.0 * cross_prod))


def reference(points, targets, start, interp, skel_points, near_leaves, near_count):
    subtree_leaves = LEAF_DEV * N_NARROW
    blocks = points.reshape(N_WIDE, subtree_leaves, LEAF, DIM)
    near_lists = near_leaves.reshape(N_WIDE, subtree_leaves, NEAR)
    live_mask = (jnp.arange(NEAR, dtype=jnp.int32)[None, :] < near_count[:, None]).astype(jnp.float32)
    live_mask = live_mask.reshape(N_WIDE, subtree_leaves, NEAR)
    interp_blocks = interp.reshape(N_WIDE, subtree_leaves * LEAF, RANK)
    owner_node = jnp.arange(N_WIDE * RANK, dtype=jnp.int32) // RANK
    groups = jnp.arange(N_WIDE, dtype=jnp.int32)

    def apply_kernel(weights):
        grouped = weights.reshape(RHS, N_WIDE, subtree_leaves * LEAF)
        skel_table = jnp.einsum('rgp,gpk->rgk', grouped, interp_blocks, precision=highest)
        skel_table = skel_table.reshape(RHS, N_WIDE * RANK)

        def one_group(inputs):
            leaf_points, near_ids, group_mask, group_weights, group_index = inputs
            neighbours = leaf_points[near_ids]
            cross_prod = jnp.einsum('spd,skqd->skpq', leaf_points, neighbours, precision=highest)
            own_sq = jnp.sum(leaf_points * leaf_points, axis=-1)
            near_sq = jnp.sum(neighbours * neighbours, axis=-1)
            distance = own_sq[:, None, :, None] + near_sq[:, :, None, :] - 2.0 * cross_prod
            near_kern = jnp.exp(-(kernel_rate / DIM) * distance) * group_mask[:, :, None, None]
            picked = group_weights.reshape(RHS, subtree_leaves, LEAF)[:, near_ids]
            near_term = jnp.einsum('skpq,rskq->rsp', near_kern, picked, precision=highest)
            near_term = near_term.reshape(RHS, subtree_leaves * LEAF)
            far_table = jnp.where((owner_node == group_index)[None, :], jnp.float32(0.0), skel_table)
            far_kern = kernel(leaf_points.reshape(subtree_leaves * LEAF, DIM), skel_points)
            far_term = jnp.einsum('rs,ps->rp', far_table, far_kern, precision=highest)
            return near_term + far_term

        group_terms = lax.map(one_group, (blocks, near_lists, live_mask, jnp.transpose(grouped, (1, 0, 2)), groups))
        return jnp.transpose(group_terms, (1, 0, 2)).reshape(RHS, POINTS)

    weights = start
    residual = targets
    for iteration in range(ITERS):
        residual = targets - (ridge_shift * weights + apply_kernel(weights))
        weights = weights + step_size * residual
    return weights, residual
```

```python
import jax
import jax.numpy as jnp
from jax import lax
from jax.sharding import PartitionSpec as P

ITERS = 2

ridge_shift = 1.0
step_size = 0.05
kernel_rate = 2.0
high = lax.Precision.HIGH


def swap(block, axis, count, offset):
    return lax.ppermute(block, axis, [(i, i ^ offset) for i in range(count)])


def narrow_peers(block, count):
    return [swap(block, "narrow", count, k) for k in range(1, count)]


def wide_chips(block, count):
    return [swap(block, "wide", count, k) for k in range(2, count, 2)]


def kernel_cols(sources, own, features):
    cross = lax.dot_general(
        sources, own, (((1,), (1,)), ((), ())), precision=high, preferred_element_type=jnp.float32
    )
    source_sq = jnp.sum(sources * sources, axis=1)
    own_sq = jnp.sum(own * own, axis=1)
    return jnp.exp(-(kernel_rate / features) * (source_sq[:, None] + own_sq[None, :] - 2.0 * cross))


def on_device(wide, narrow, points, targets, start, interp, skel_points, near_leaves, near_count):
    leaf_dev, near_slots = near_leaves.shape
    rows, features = points.shape
    leaf = rows // leaf_dev
    rhs = targets.shape[0]
    rank = interp.shape[1]
    me = lax.axis_index("narrow")

    def partial_skel(weights):
        return jnp.dot(weights, interp, precision=high, preferred_element_type=jnp.float32)

    def spread(weights):
        pack = jnp.concatenate([weights, partial_skel(weights)], axis=1)
        got = narrow_peers(pack, narrow)
        sub = jnp.concatenate([weights] + [g[:, :rows] for g in got], axis=1)
        table = pack[:, rows:]
        for g in got:
            table = table + g[:, rows:]
        chips = jnp.concatenate([table] + wide_chips(table, wide), axis=0)
        other = swap(chips, "wide", wide, 1)
        both = jnp.concatenate([chips[rhs:], other], axis=0)
        both = both.reshape(wide - 1, rhs, rank).transpose(1, 0, 2).reshape(rhs, (wide - 1) * rank)
        return jnp.concatenate([sub, both], axis=1)

    first = spread(start)
    skel_chips = jnp.concatenate([skel_points] + wide_chips(skel_points, wide), axis=0)
    skel_other = swap(skel_chips, "wide", wide, 1)
    skels = jnp.concatenate([skel_chips[rank:], skel_other], axis=0)
    subtree = jnp.concatenate([points] + narrow_peers(points, narrow), axis=0)

    live = jnp.arange(near_slots, dtype=jnp.int32)[None, :] < near_count[:, None]
    owner = jnp.arange(narrow, dtype=jnp.int32) ^ me
    leaf_ids = (owner[:, None] * leaf_dev + jnp.arange(leaf_dev, dtype=jnp.int32)[None, :]).reshape(-1)
    named = (near_leaves[None, :, :] == leaf_ids[:, None, None]) & live[None]
    mask = jnp.sum(named.astype(jnp.float32), axis=-1)
    near_kern = kernel_cols(subtree, points, features).reshape(narrow * leaf_dev, leaf, leaf_dev, leaf)
    near_kern = (near_kern * mask[:, None, :, None]).reshape(narrow * rows, rows)
    far_kern = kernel_cols(skels, points, features)
    kern = jnp.concatenate([near_kern, far_kern], axis=0)

    weights = start
    table = first
    for iteration in range(ITERS):
        if iteration:
            table = spread(weights)
        applied = jnp.dot(table, kern, precision=high, preferred_element_type=jnp.float32)
        residual = targets - (ridge_shift * weights + applied)
        weights = weights + step_size * residual
    return (weights, residual)


def solution(mesh):
    wide, narrow = mesh.shape["wide"], mesh.shape["narrow"]

    def body(*args):
        return on_device(wide, narrow, *args)

    in_specs = (
        P(("wide", "narrow"), None),
        P(None, ("wide", "narrow")),
        P(None, ("wide", "narrow")),
        P(("wide", "narrow"), None),
        P("wide", None),
        P(("wide", "narrow"), None),
        P(("wide", "narrow")),
    )
    out_specs = (P(None, ("wide", "narrow")), P(None, ("wide", "narrow")))
    return jax.shard_map(body, mesh=mesh, in_specs=in_specs, out_specs=out_specs, check_vma=False)
```

```python
import functools

import jax
import jax.numpy as jnp
from jax import lax
from jax.experimental import pallas as pl
from jax.experimental.pallas import tpu as pltpu
from jax.sharding import PartitionSpec as P


ITERS = 2

ridge_shift = 1.0
step_size = 0.05
kernel_rate = 2.0


VMEM = pl.BlockSpec(memory_space=pltpu.VMEM)
f32, bf16 = jnp.float32, jnp.bfloat16


def swap(block, axis, count, offset):
    return lax.ppermute(block, axis, [(i, i ^ offset) for i in range(count)])


def narrow_peers(block, count):
    return [swap(block, "narrow", count, k) for k in range(1, count)]


def wide_chips(block, count):
    return [swap(block, "wide", count, k) for k in range(2, count, 2)]


def limit_of(args, outs):
    sizes = [a.size * a.dtype.itemsize for a in list(args) + jax.tree.leaves(outs)]
    return 2 * sum(sizes) + (4 << 20)


def call(body, out_shape, flops, *args):
    return pl.pallas_call(
        body,
        out_shape=out_shape,
        in_specs=[VMEM] * len(args),
        out_specs=jax.tree.map(lambda _: VMEM, out_shape),
        compiler_params=pltpu.CompilerParams(vmem_limit_bytes=limit_of(args, out_shape)),
        cost_estimate=pl.CostEstimate(flops=flops, bytes_accessed=1 << 20, transcendentals=0),
    )(*args)


def halves(values):
    upper = values.astype(bf16)
    return upper, (values - upper.astype(f32)).astype(bf16)


def mm(left, right, right_dim=0):
    return lax.dot_general(
        left, right, (((1,), (right_dim,)), ((), ())), preferred_element_type=f32
    )


def dot3(left, upper, lower, right_dim=0):
    left_upper, left_lower = halves(left)
    return (
        mm(left_upper, upper, right_dim)
        + mm(left_lower, upper, right_dim)
        + mm(left_upper, lower, right_dim)
    )


def pack_body(points, start, interp, skels, out, upper, lower, skels_out, weights, maps, sems):
    rows, _ = points.shape
    moves = [
        pltpu.make_async_copy(start, weights, sems.at[0]),
        pltpu.make_async_copy(interp, maps, sems.at[1]),
        pltpu.make_async_copy(points, out.at[pl.ds(0, rows)], sems.at[2]),
        pltpu.make_async_copy(skels, skels_out, sems.at[3]),
    ]
    for move in moves:
        move.start()
    moves[0].wait()
    moves[1].wait()
    upper[...], lower[...] = halves(maps[...])
    put_weights(out, rows, weights[...], dot3(weights[...], upper[...], lower[...]))
    moves[2].wait()
    moves[3].wait()


def put_weights(out, at, weights, partial):
    rhs, rows = weights.shape
    width = out.shape[1]
    for begin in range(0, rows, width):
        out[at : at + rhs] = weights[:, begin : begin + width]
        at += rhs
    out[at : at + rhs] = partial


def own_terms(own, features):
    scaled = own * (2.0 * kernel_rate / features)
    ones = jnp.ones((8, features), f32)
    norms = lax.dot_general(
        ones, own * own, (((1,), (1,)), ((), ())),
        precision=lax.Precision.HIGHEST, preferred_element_type=f32,
    )[:1] * (-kernel_rate / features)
    return halves(scaled) + (norms,)


def columns(sources, terms, features):
    upper, lower, norms = terms
    source_norms = jnp.sum(sources * sources, axis=1, keepdims=True) * (-kernel_rate / features)
    return jnp.exp(dot3(sources, upper, lower, 1) + source_norms + norms)


def store(values, at, upper, lower):
    high, low = halves(values)
    upper[at : at + values.shape[0]] = high
    lower[at : at + values.shape[0]] = low


def near_body(rows, near_leaves, near_count, *refs):
    packs, (upper, lower) = refs[:-2], refs[-2:]
    leaf_dev, features = near_leaves.shape[0], packs[0].shape[1]
    leaf = rows // leaf_dev
    me = lax.axis_index("narrow")
    terms = own_terms(packs[0][:rows], features)
    names = near_leaves[...]
    live = lax.broadcasted_iota(jnp.int32, names.shape, 1) < near_count[...]
    for offset, block in enumerate(packs):
        for row in range(leaf_dev):
            named = live & (names == (me ^ offset) * leaf_dev + row)
            held = jnp.sum(named.astype(f32), axis=1, keepdims=True)
            mask = jnp.concatenate(
                [jnp.broadcast_to(held[i : i + 1], (1, leaf)) for i in range(leaf_dev)], axis=1
            )
            part = block[row * leaf : (row + 1) * leaf]
            at = offset * rows + row * leaf
            store(columns(part, terms, features) * mask, at, upper, lower)


def far_body(rows, pack, *refs):
    blocks, (upper, lower) = refs[:-2], refs[-2:]
    features = pack.shape[1]
    terms = own_terms(pack[:rows], features)
    at = 0
    for block in blocks:
        store(columns(block[...], terms, features), at, upper, lower)
        at += block.shape[0]


def residual_of(narrow, chips, targets, refs):
    packs, tables = refs[:narrow], refs[narrow : narrow + chips - 1]
    first, others, near_upper, near_lower, far_upper, far_lower = refs[narrow + chips - 1 :]
    rhs, rows = targets.shape
    width = packs[0].shape[1]
    blocks = rows // width
    total = jnp.zeros((2 * rhs, rows), f32)
    small = jnp.zeros((rhs, rows), f32)
    parts = []
    for i, pack in enumerate(packs):
        at = pack.shape[0] - (blocks + 1) * rhs
        for j in range(blocks):
            values = pack[at + j * rhs : at + (j + 1) * rhs]
            parts.append((values, near_upper, near_lower, i * rows + j * width))
    own = jnp.concatenate([part[0] for part in parts[:blocks]], axis=1)
    far = [t[...] for t in tables] + [first[...]]
    far += [others[i * rhs : (i + 1) * rhs] for i in range(chips - 1)]
    parts += [(t, far_upper, far_lower, i * t.shape[1]) for i, t in enumerate(far)]
    for values, upper, lower, at in parts:
        high, low = halves(values)
        depth = values.shape[1]
        total = total + mm(jnp.concatenate([high, low], axis=0), upper[at : at + depth])
        small = small + mm(high, lower[at : at + depth])
    applied = total[:rhs] + total[rhs:] + small
    residual = targets[...] - (ridge_shift * own + applied)
    return own + step_size * residual, residual


def next_body(narrow, chips, targets, upper, lower, *refs):
    weights, _ = residual_of(narrow, chips, targets, refs[:-1])
    put_weights(refs[-1], 0, weights, dot3(weights, upper[...], lower[...]))


def last_body(narrow, chips, targets, *refs):
    refs[-2][...], refs[-1][...] = residual_of(narrow, chips, targets, refs[:-2])


def on_device(wide, narrow, points, targets, start, interp, skel_points, near_leaves, near_count):
    rows, features = points.shape
    rhs = targets.shape[0]
    rank = interp.shape[1]
    if rank != features or rows % features:
        raise ValueError("unexpected shapes")
    chips = wide // 2
    unit = 6 * rows * features
    moved = (rows // features + 1) * rhs

    def partner(block):
        return swap(block, "wide", wide, 1)

    def spread(pack):
        packs = [pack] + narrow_peers(pack, narrow)
        table = sum(p[p.shape[0] - rhs :] for p in packs)
        tables = wide_chips(table, wide)
        first = partner(table)
        others = partner(jnp.concatenate(tables, axis=0))
        return packs, tables + [first, others]

    def pair(count, width):
        return (jax.ShapeDtypeStruct((count, width), bf16),) * 2

    flat = jax.ShapeDtypeStruct((rhs, rows), f32)
    pack, upper, lower, skel_own = pl.pallas_call(
        pack_body,
        out_shape=(jax.ShapeDtypeStruct((rows + moved, features), f32),)
        + pair(rows, rank)
        + (jax.ShapeDtypeStruct(skel_points.shape, f32),),
        in_specs=[pl.BlockSpec(memory_space=pltpu.HBM)] * 4,
        out_specs=(VMEM,) * 4,
        scratch_shapes=[
            pltpu.VMEM((rhs, rows), f32),
            pltpu.VMEM((rows, rank), f32),
            pltpu.SemaphoreType.DMA((4,)),
        ],
        compiler_params=pltpu.CompilerParams(vmem_limit_bytes=8 << 20),
        cost_estimate=pl.CostEstimate(
            flops=6 * rhs * rows * rank, bytes_accessed=4 * rows * rank, transcendentals=0
        ),
    )(*[pltpu.with_memory_space_constraint(a, pltpu.HBM) for a in (points, start, interp, skel_points)])
    maps = (upper, lower)
    packs, sent = spread(pack)
    skels = wide_chips(skel_own, wide)
    skel_chips = jnp.concatenate(skels, axis=0)
    skels = skels + [partner(skel_own), partner(skel_chips)]
    near = call(
        functools.partial(near_body, rows), pair(narrow * rows, rows), unit * narrow * rows,
        near_leaves, near_count[:, None], *packs,
    )
    far = call(
        functools.partial(far_body, rows), pair((wide - 1) * rank, rows),
        unit * (wide - 1) * rank, pack, *skels,
    )
    apply_flops = 6 * rhs * rows * (narrow * rows + wide * rank)
    for _ in range(ITERS - 1):
        pack = call(
            functools.partial(next_body, narrow, chips),
            jax.ShapeDtypeStruct((moved, features), f32), apply_flops,
            targets, *maps, *packs, *sent, *near, *far,
        )
        packs, sent = spread(pack)
    return call(
        functools.partial(last_body, narrow, chips), (flat, flat), apply_flops,
        targets, *packs, *sent, *near, *far,
    )


def solution(mesh):
    wide, narrow = mesh.shape["wide"], mesh.shape["narrow"]

    def body(*args):
        return on_device(wide, narrow, *args)

    in_specs = (
        P(("wide", "narrow"), None),
        P(None, ("wide", "narrow")),
        P(None, ("wide", "narrow")),
        P(("wide", "narrow"), None),
        P("wide", None),
        P(("wide", "narrow"), None),
        P(("wide", "narrow")),
    )
    out_specs = (P(None, ("wide", "narrow")), P(None, ("wide", "narrow")))
    return jax.shard_map(body, mesh=mesh, in_specs=in_specs, out_specs=out_specs, check_vma=False)
```

```python
import functools
import math

import jax
import jax.numpy as jnp
from jax import lax
from jax.experimental import pallas as pl
from jax.experimental.pallas import tpu as pltpu
from jax.sharding import PartitionSpec as P


ITERS = 2

ridge_shift = 1.0
step_size = 0.05
kernel_rate = 2.0
rate2 = kernel_rate / math.log(2.0)


VMEM = pl.BlockSpec(memory_space=pltpu.VMEM)
f32, bf16 = jnp.float32, jnp.bfloat16


def swap(block, axis, count, offset):
    return lax.ppermute(block, axis, [(i, i ^ offset) for i in range(count)])


def narrow_peers(block, count, step=1):
    return [swap(block, "narrow", count, k) for k in range(step, count, step)]


def wide_chips(block, count):
    return [swap(block, "wide", count, k) for k in range(2, count, 2)]


def limit_of(args, outs):
    sizes = [a.size * a.dtype.itemsize for a in list(args) + jax.tree.leaves(outs)]
    return 3 * sum(sizes) + (4 << 20)


def call(body, out_shape, flops, *args, scratch=()):
    return pl.pallas_call(
        body,
        out_shape=out_shape,
        in_specs=[VMEM] * len(args),
        out_specs=jax.tree.map(lambda _: VMEM, out_shape),
        scratch_shapes=scratch,
        compiler_params=pltpu.CompilerParams(vmem_limit_bytes=limit_of(args, out_shape)),
        cost_estimate=pl.CostEstimate(flops=flops, bytes_accessed=1 << 20, transcendentals=0),
    )(*args)


def halves(values):
    upper = values.astype(bf16)
    return upper, (values - upper.astype(f32)).astype(bf16)


def mm(left, right, right_dim=0):
    return lax.dot_general(
        left, right, (((1,), (right_dim,)), ((), ())), preferred_element_type=f32
    )


def dot3(left, upper, lower, right_dim=0):
    left_upper, left_lower = halves(left)
    return (
        mm(left_upper, upper, right_dim)
        + mm(left_lower, upper, right_dim)
        + mm(left_upper, lower, right_dim)
    )


def pack_body(
    points, start, interp, skels, targets, near_leaves, near_count,
    zpack, npack, xpack, weights, goals, names, counts, sems,
):
    rows, features = points.shape
    rank = skels.shape[0]
    leaf_dev, slots = near_leaves.shape
    moves = [
        pltpu.make_async_copy(start, weights, sems.at[0]),
        pltpu.make_async_copy(interp, xpack.at[pl.ds(0, rows)], sems.at[1]),
        pltpu.make_async_copy(skels, zpack.at[pl.ds(0, rank)], sems.at[2]),
        pltpu.make_async_copy(points, npack.at[pl.ds(0, rows)], sems.at[3]),
        pltpu.make_async_copy(targets, goals, sems.at[4]),
        pltpu.make_async_copy(near_leaves, names, sems.at[5]),
        pltpu.make_async_copy(near_count, counts, sems.at[6]),
    ]
    for move in moves:
        move.start()
    for move in moves:
        move.wait()
    zpack[rank:] = dot3(weights[...], *halves(xpack[:rows]))
    put_blocks(npack, rows, weights[...])
    slot = lax.broadcasted_iota(jnp.int32, (1, slots), 1)
    npack[npack.shape[0] - 8 :] = jnp.full((8, features), -1.0, f32)
    for i in range(leaf_dev):
        live = jnp.where(slot < counts[i], names[i : i + 1].astype(f32), -1.0)
        npack[pl.ds(npack.shape[0] - 8 + i, 1), pl.ds(0, slots)] = live
    put_blocks(xpack, rows, goals[...])


def put_blocks(out, at, values):
    rhs, rows = values.shape
    width = out.shape[1]
    for begin in range(0, rows, width):
        out[at : at + rhs] = values[:, begin : begin + width]
        at += rhs


def get_blocks(ref, at, rhs, rows):
    width = ref.shape[1]
    return [ref[at + i * rhs : at + (i + 1) * rhs] for i in range(rows // width)]


def own_terms(own, features):
    scaled = own * (2.0 * rate2 / features)
    ones = jnp.ones((8, features), f32)
    norms = lax.dot_general(
        ones, own * own, (((1,), (1,)), ((), ())),
        precision=lax.Precision.HIGHEST, preferred_element_type=f32,
    )[:1] * (-rate2 / features)
    upper, lower = halves(scaled)
    return jnp.concatenate([upper, upper, lower], axis=1), norms


def kernel_pair(sources, owns, gates, upper_out, lower_out, triples, own_triples, cross):
    features = owns[0].shape[1]
    rows = owns[0].shape[0]
    own_norms = []
    for half, own in enumerate(owns):
        own_triples[half * rows : (half + 1) * rows], norms = own_terms(own, features)
        own_norms.append(norms)
    norms = jnp.concatenate(own_norms, axis=1)
    at = 0
    for source in sources:
        upper, lower = halves(source)
        triples[at : at + source.shape[0]] = jnp.concatenate([upper, lower, upper], axis=1)
        at += source.shape[0]
    cross[...] = mm(triples[...], own_triples[...], 1)
    at = 0
    for i, source in enumerate(sources):
        here = slice(at, at + source.shape[0])
        source_norms = jnp.sum(source * source, axis=1, keepdims=True) * (-rate2 / features)
        side = norms if gates is None else norms + gates[i]
        upper_out[here], lower_out[here] = halves(jnp.exp2(cross[here] + source_norms + side))
        at += source.shape[0]


def near_body(rows, leaf_dev, *refs):
    packs, rest = refs[:-5], refs[-5:]
    leaf = rows // leaf_dev
    me = lax.axis_index("narrow")
    names = [packs[half][packs[half].shape[0] - 8 :][:leaf_dev] for half in range(2)]
    sources, gates = [], []
    for offset, block in enumerate(packs):
        for row in range(leaf_dev):
            wanted = ((me ^ offset) * leaf_dev + row).astype(f32)
            sides = []
            for half in range(2):
                held = jnp.sum((names[half] == wanted).astype(f32), axis=1, keepdims=True)
                gate = jnp.where(held > 0.0, 0.0, -jnp.inf)
                sides += [jnp.broadcast_to(gate[i : i + 1], (1, leaf)) for i in range(leaf_dev)]
            gates.append(jnp.concatenate(sides, axis=1))
            sources.append(block[row * leaf : (row + 1) * leaf])
    kernel_pair(sources, [p[:rows] for p in packs[:2]], gates, *rest)


def collect_body(*refs):
    zpacks, (skels, partials) = refs[:-2], refs[-2:]
    rank = skels.shape[0] // len(zpacks)
    rhs = partials.shape[0] // len(zpacks)
    for i, pack in enumerate(zpacks):
        skels[i * rank : (i + 1) * rank] = pack[:rank]
        partials[i * rhs : (i + 1) * rhs] = pack[rank:]


def far_body(rows, rank, own, beside, skels, others, *rest):
    sources = [skels[i : i + rank] for i in range(rank, skels.shape[0], rank)]
    sources += [others[i : i + rank] for i in range(0, others.shape[0], rank)]
    kernel_pair(sources, [own[:rows], beside[:rows]], None, *rest)


def applied_to(parts, cols):
    rhs = parts[0][0].shape[0]
    width = cols.stop - cols.start
    total = jnp.zeros((2 * rhs, width), f32)
    small = jnp.zeros((rhs, width), f32)
    for values, upper, lower, at in parts:
        high, low = halves(values)
        depth = values.shape[1]
        total = total + mm(jnp.concatenate([high, low], axis=0), upper[at : at + depth, cols])
        small = small + mm(high, lower[at : at + depth, cols])
    return total[:rhs] + total[rhs:] + small


def all_parts(near_blocks, far_blocks, kern):
    near_upper, near_lower, far_upper, far_lower = kern
    parts = [(v, near_upper, near_lower, i * v.shape[1]) for i, v in enumerate(near_blocks)]
    return parts + [(v, far_upper, far_lower, i * v.shape[1]) for i, v in enumerate(far_blocks)]


def stepped(own, goals, applied):
    residual = goals - (ridge_shift * own + applied)
    return own + step_size * residual, residual


def next_body(narrow, xpack, beside, *refs):
    packs, (tables, others), kern, out = refs[:narrow], refs[narrow : narrow + 2], refs[-5:-1], refs[-1]
    rank = xpack.shape[1]
    cols = kern[0].shape[1]
    rows = cols // 2
    blocks = rows // rank
    rhs = (xpack.shape[0] - rows) // blocks
    near = [get_blocks(p, rows, rhs, rows) for p in packs]
    far = [tables[i : i + rhs] for i in range(rhs, tables.shape[0], rhs)]
    far += [others[i : i + rhs] for i in range(0, others.shape[0], rhs)]
    applied = applied_to(all_parts(sum(near, []), far, kern), slice(0, cols))
    own = jnp.concatenate(near[0] + near[1], axis=1)
    goals = get_blocks(xpack, rows, rhs, rows) + get_blocks(beside, rows, rhs, rows)
    weights, _ = stepped(own, jnp.concatenate(goals, axis=1), applied)
    put_blocks(out, 0, weights)
    out[2 * blocks * rhs :] = dot3(weights[:, :rows], *halves(xpack[:rows])) + dot3(
        weights[:, rows:], *halves(beside[:rows])
    )


def last_body(pairs, chips, xpack, *refs):
    packs, tables = refs[:pairs], refs[pairs : pairs + chips - 1]
    others = refs[pairs + chips - 1]
    kern, (weights_out, residual_out) = refs[-6:-2], refs[-2:]
    rhs, rows = weights_out.shape
    near = [get_blocks(p, 0, rhs, 2 * rows) for p in packs]
    far = [t[...] for t in tables] + [others[i : i + rhs] for i in range(0, others.shape[0], rhs)]
    applied = applied_to(all_parts(sum(near, []), far, kern), slice(0, rows))
    own = jnp.concatenate(get_blocks(packs[0], 0, rhs, rows), axis=1)
    goals = jnp.concatenate(get_blocks(xpack, rows, rhs, rows), axis=1)
    weights_out[...], residual_out[...] = stepped(own, goals, applied)


def on_device(wide, narrow, points, targets, start, interp, skel_points, near_leaves, near_count):
    rows, features = points.shape
    rhs = targets.shape[0]
    rank = interp.shape[1]
    leaf_dev, _ = near_leaves.shape
    if rank != features or rows % features or leaf_dev > 8 or narrow % 2 or ITERS != 2:
        raise ValueError("unexpected shapes")
    chips = wide // 2
    blocks = rows // features
    unit = 12 * rows * features

    def partner(block):
        return swap(block, "wide", wide, 1)

    def vmem(height):
        return jax.ShapeDtypeStruct((height, features), f32)

    def pair(count):
        return (jax.ShapeDtypeStruct((count, 2 * rows), bf16),) * 2

    inputs = (points, start, interp, skel_points, targets, near_leaves, near_count)
    zpack, npack, xpack = pl.pallas_call(
        pack_body,
        out_shape=(vmem(rank + rhs), vmem(rows + blocks * rhs + 8), vmem(rows + blocks * rhs)),
        in_specs=[pl.BlockSpec(memory_space=pltpu.HBM)] * len(inputs),
        out_specs=(VMEM,) * 3,
        scratch_shapes=[
            pltpu.VMEM((rhs, rows), f32),
            pltpu.VMEM((rhs, rows), f32),
            pltpu.VMEM(near_leaves.shape, jnp.int32),
            pltpu.SMEM(near_count.shape, jnp.int32),
            pltpu.SemaphoreType.DMA((len(inputs),)),
        ],
        compiler_params=pltpu.CompilerParams(vmem_limit_bytes=8 << 20),
        cost_estimate=pl.CostEstimate(
            flops=6 * rhs * rows * rank, bytes_accessed=4 * rows * rank, transcendentals=0
        ),
    )(*[pltpu.with_memory_space_constraint(a, pltpu.HBM) for a in inputs])

    def staged(axis, block, count, offset):
        return swap(block, axis, count, offset)

    npacks = [npack] + [staged("narrow", npack, narrow, k) for k in range(1, narrow)]
    zpacks = [zpack] + [staged("wide", zpack, wide, k) for k in range(2, wide, 2)]
    skels, partials = call(
        collect_body, (vmem(chips * rank), vmem(chips * rhs)), chips * rank * features, *zpacks
    )
    tables = sum(narrow_peers(partials, narrow), partials)
    beside = swap(xpack, "narrow", narrow, 1)
    skel_others = partner(skels)
    table_others = partner(tables)

    def room(count):
        return (
            pltpu.VMEM((count, 3 * features), bf16),
            pltpu.VMEM((2 * rows, 3 * features), bf16),
            pltpu.VMEM((count, 2 * rows), f32),
        )

    near = call(
        functools.partial(near_body, rows, leaf_dev), pair(narrow * rows),
        unit * narrow * rows, *npacks, scratch=room(narrow * rows),
    )
    far = call(
        functools.partial(far_body, rows, rank), pair((wide - 1) * rank),
        unit * (wide - 1) * rank, npacks[0], npacks[1], skels, skel_others,
        scratch=room((wide - 1) * rank),
    )
    apply_flops = 12 * rhs * rows * (narrow * rows + wide * rank)
    pack = call(
        functools.partial(next_body, narrow), vmem((2 * blocks + 1) * rhs), apply_flops,
        xpack, beside, *npacks, tables, table_others, *near, *far,
    )
    packs = [pack] + narrow_peers(pack, narrow, 2)
    table = sum(p[2 * blocks * rhs :] for p in packs)
    later = wide_chips(table, wide)
    later_others = partner(jnp.concatenate([table] + later, axis=0))
    flat = jax.ShapeDtypeStruct((rhs, rows), f32)
    return call(
        functools.partial(last_body, narrow // 2, chips), (flat, flat), apply_flops // 2,
        xpack, *packs, *later, later_others, *near, *far,
    )


def solution(mesh):
    wide, narrow = mesh.shape["wide"], mesh.shape["narrow"]

    def body(*args):
        return on_device(wide, narrow, *args)

    in_specs = (
        P(("wide", "narrow"), None),
        P(None, ("wide", "narrow")),
        P(None, ("wide", "narrow")),
        P(("wide", "narrow"), None),
        P("wide", None),
        P(("wide", "narrow"), None),
        P(("wide", "narrow")),
    )
    out_specs = (P(None, ("wide", "narrow")), P(None, ("wide", "narrow")))
    return jax.shard_map(body, mesh=mesh, in_specs=in_specs, out_specs=out_specs, check_vma=False)
```
